256 devices in a mesh: blk: 128 (over x, z, y_hi, core), rep: 2 (over y_lo).
Axes of the slice: x: 4, y: 4 (y_hi: 2, y_lo: 2; y = y_hi * 2 + y_lo), z: 8, core: 2. Of those that a mesh axis runs over, the one named last changes fastest.
Arguments:
- frames: bfloat16 [2, 6144, 384], P('rep', 'blk'), may hold values from -600 to 600
- codebook: bfloat16 [131072, 384], P('blk'), may hold values from -2 to 2
Outputs:
- log_total: float32 [2, 6144], P('rep', 'blk')
- counts: float32 [131072], P('blk')
- entropy: float32 [], replicated
The draws below stay inside these ranges and needn't reach their ends.
All inputs are finite; a program needn't handle non-finite values.
Results may differ from the reference program's by a relative error of at most 0.00065.
Values may be sent and summed in bfloat16 or wider, within the bound.
No kernel may reach another device: no remote copies, remote signals or barrier semaphores. Data moves between devices by JAX's collectives and lax.ppermute only.
A program may use at most 128 MiB of HBM per device.

```python
import math
import jax
import jax.numpy as jnp
from jax import lax

D = 384
V_DEV = 1024
GROUPS = 2
FR_GROUP = 6144
FRAMES = 12288
CODEBOOK = 131072
N_BLK = 128


def draw_codebook(key, part):
    rough_key, value_key = jax.random.split(jax.random.fold_in(key, 23))
    ladder = jnp.arange(CODEBOOK, dtype=jnp.float32) / CODEBOOK
    ramp = 0.6 * jnp.exp(ladder * math.log(3.0))
    rough = jnp.exp(jax.random.uniform(rough_key, (CODEBOOK,), jnp.float32, math.log(0.7), math.log(1.4)))
    values = jax.random.truncated_normal(value_key, -4.0, 4.0, (CODEBOOK, D), jnp.float32)
    scaled = values * (ramp * rough)[:, None] / math.sqrt(D)
    return scaled.astype(jnp.bfloat16)


def draw_frames(key, part):
    keys = jax.random.split(jax.random.fold_in(key, 11), 2)
    row_scale = jnp.exp(jax.random.uniform(keys[0], (GROUPS, FR_GROUP, 1), jnp.float32, math.log(0.3), math.log(3.0)))
    values = jax.random.truncated_normal(keys[1], -4.0, 4.0, (GROUPS, FR_GROUP, D), jnp.float32)
    result = values * row_scale
    return result.astype(jnp.bfloat16)


def setup_inputs(seed: int = 0) -> dict:
    splits = jax.random.split(jax.random.key(seed), 3)
    frames = draw_frames(jax.random.fold_in(splits[2], 71), 0)
    codebook = draw_codebook(jax.random.fold_in(splits[2], 71), 0)
    return dict(frames=frames, codebook=codebook)


def shard_scores(frame_rows, weights):
    return lax.dot_general(frame_rows, weights, (((1,), (1,)), ((), ())), preferred_element_type=jnp.float32)


def group_pass(frame_rows, codebook):
    shards = codebook.reshape(N_BLK, V_DEV, D)

    def stat_step(carried, weights):
        high, total = carried
        scores = shard_scores(frame_rows, weights)
        new_high = jnp.maximum(high, jnp.max(scores, axis=1))
        new_total = total * jnp.exp(high - new_high) + jnp.sum(jnp.exp(scores - new_high[:, None]), axis=1)
        return (new_high, new_total), None

    start_high = jnp.full((FR_GROUP,), -jnp.inf, jnp.float32)
    start_total = jnp.zeros((FR_GROUP,), jnp.float32)
    (row_high, row_total), _ = lax.scan(stat_step, (start_high, start_total), shards)
    row_lse = row_high + jnp.log(row_total)

    def shard_usage(weights):
        scores = shard_scores(frame_rows, weights)
        return jnp.sum(jnp.exp(scores - row_lse[:, None]), axis=0)

    usage = lax.map(shard_usage, shards).reshape(CODEBOOK)
    return row_lse, usage


def reference(frames, codebook):
    lse_list = []
    usage_total = jnp.zeros((CODEBOOK,), jnp.float32)
    for member in range(GROUPS):
        row_lse, usage = group_pass(frames[member], codebook)
        lse_list.append(row_lse)
        usage_total = usage_total + usage
    mean_use = usage_total / FRAMES
    entropy = -jnp.sum(mean_use * jnp.log(mean_use + 1e-7))
    return jnp.stack(lse_list, axis=0), usage_total, entropy
```

```python
import functools

import jax
import jax.numpy as jnp
from jax import lax
from jax.experimental import pallas as pl
from jax.experimental.pallas import tpu as pltpu
from jax.sharding import Mesh
from jax.sharding import PartitionSpec as P

BLK = ("x", "z", "yh", "core")
RING_Y = ("yh", "rep")
COLUMN = ("yh", "core", "rep")
PLANE = ("x", "z")
LOG2E = 1.4426950408889634
VB = 256
FB = 256


def spread(array, axis):
    n = lax.axis_size(axis)
    copies = jnp.broadcast_to(array, (n, *array.shape))
    return lax.all_to_all(copies, axis, split_axis=0, concat_axis=0, tiled=True)


def tile_kernel(frames_ref, codes_ref, probs_ref, high_ref, total_ref):
    blocks = codes_ref.shape[0] // VB

    def scores_of(k):
        return lax.dot_general(
            codes_ref[pl.ds(k * VB, VB), :],
            frames_ref[...],
            (((1,), (1,)), ((), ())),
            preferred_element_type=jnp.float32,
        )

    for k in range(blocks):
        s = scores_of(k)
        high = jnp.max(s, axis=0, keepdims=True)
        p = jnp.exp2((s - high) * LOG2E)
        probs_ref[pl.ds(k * VB, VB), :] = p
        high_ref[pl.ds(k, 1), :] = high
        total_ref[pl.ds(k, 1), :] = jnp.sum(p, axis=0, keepdims=True)


def tile_stats(frames, codes):
    rows, width = frames.shape
    protos = codes.shape[0]
    blocks = protos // VB
    return pl.pallas_call(
        tile_kernel,
        grid=(rows // FB,),
        in_specs=[
            pl.BlockSpec((FB, width), lambda i: (i, 0)),
            pl.BlockSpec((protos, width), lambda i: (0, 0)),
        ],
        out_specs=[
            pl.BlockSpec((protos, FB), lambda i: (0, i)),
            pl.BlockSpec((blocks, FB), lambda i: (0, i)),
            pl.BlockSpec((blocks, FB), lambda i: (0, i)),
        ],
        out_shape=[
            jax.ShapeDtypeStruct((protos, rows), jnp.float32),
            jax.ShapeDtypeStruct((blocks, rows), jnp.float32),
            jax.ShapeDtypeStruct((blocks, rows), jnp.float32),
        ],
        compiler_params=pltpu.CompilerParams(
            dimension_semantics=("arbitrary",), vmem_limit_bytes=24 * 1024 * 1024
        ),
        cost_estimate=pl.CostEstimate(
            flops=2 * rows * protos * width,
            bytes_accessed=4 * rows * protos + 2 * (rows + protos) * width,
            transcendentals=rows * protos,
        ),
        name="tile_stats",
    )(frames, codes)


def absolute_order(parts, yh, core):
    parts = jnp.where(yh == 1, parts[::-1], parts)
    return jnp.where(core == 1, parts[:, ::-1], parts)


def per_device(frames, codebook):
    own = frames[0]
    shard_rows, width = own.shape
    owned = codebook.shape[0]
    yh, core = lax.axis_index("yh"), lax.axis_index("core")

    opposite = lax.ppermute(codebook, RING_Y, [(0, 3), (3, 0), (1, 2), (2, 1)])
    both = jnp.concatenate([codebook, opposite])
    swapped = lax.ppermute(both, "core", [(0, 1), (1, 0)])
    codes = jnp.stack(
        [codebook, swapped[:owned], opposite, swapped[owned:]]
    ).reshape(-1, width)

    line = spread(own, "z").reshape(-1, width)
    rows = spread(line, "x").reshape(-1, width)

    probs, high, total = tile_stats(rows, codes)
    top = jnp.max(high, axis=0)
    part_lse = top + jnp.log(jnp.sum(total * jnp.exp(high - top), axis=0))
    parts = spread(part_lse, PLANE)
    peak = jnp.max(parts, axis=0)
    lse = peak + jnp.log(jnp.sum(jnp.exp(parts - peak), axis=0))

    weight = jnp.exp(high - lse)
    blocks = weight.shape[0]
    usage = jnp.sum(
        probs.reshape(blocks, VB, -1) * weight[:, None, :], axis=2
    ).reshape(2, 2, owned)
    usage = absolute_order(usage, yh, core).reshape(-1)
    column = jnp.sum(spread(usage, COLUMN), axis=0)

    at = (lax.axis_index(PLANE)) * shard_rows
    lse_own = lax.dynamic_slice_in_dim(lse, at, shard_rows, 0)
    usage_own = lax.dynamic_slice_in_dim(column, (2 * yh + core) * owned, owned, 0)

    embeddings = shard_rows * lax.axis_size(BLK) * lax.axis_size("rep")
    mean_use = column / embeddings
    term = -jnp.sum(mean_use * jnp.log(mean_use + 1e-07), keepdims=True)
    entropy = jnp.sum(spread(term, PLANE))
    return (lse_own[None, :], usage_own, entropy)


def solution(mesh):
    split = Mesh(
        mesh.devices.reshape(4, 8, 2, 2, mesh.shape["rep"]),
        ("x", "z", "yh", "core", "rep"),
    )
    return jax.shard_map(
        per_device,
        mesh=split,
        in_specs=(P("rep", BLK, None), P(BLK, None)),
        out_specs=(P("rep", BLK), P(BLK), P()),
        check_vma=False,
    )
```

```python
import functools

import jax
import jax.numpy as jnp
from jax import lax
from jax.experimental import pallas as pl
from jax.experimental.pallas import tpu as pltpu
from jax.sharding import Mesh
from jax.sharding import PartitionSpec as P


BLK = ("x", "z", "yh", "core")
RING_Y = ("yh", "rep")
COLUMN = ("yh", "core", "rep")
PLANE = ("x", "z")
LOG2E = 1.4426950408889634
VB = 256
FB = 256
LANES = 128


def exchange(array, axis):
    return lax.all_to_all(array, axis, split_axis=0, concat_axis=0, tiled=True)


def spread(array, axis):
    n = lax.axis_size(axis)
    return exchange(jnp.broadcast_to(array, (n, *array.shape)), axis)


def shifted(array, step):
    n = lax.axis_size("x")
    return lax.ppermute(array, "x", [(i, (i + step) % n) for i in range(n)])


def in_vmem(count):
    return [pl.BlockSpec(memory_space=pltpu.VMEM)] * count


def scores_into(scratch, codes, start, frames):
    s = lax.dot_general(
        codes[pl.ds(start, VB), :],
        frames,
        (((1,), (1,)), ((), ())),
        preferred_element_type=jnp.float32,
    )
    scratch[...] = s
    return jnp.max(s, axis=0, keepdims=True)


def tile(frames_of, chunks, width, codes, probs, high, total, scratch):
    steps = [(c, b) for c in codes for b in range(0, c.shape[0], VB)]

    def chunk(i, top):
        lanes = pl.ds(pl.multiple_of(i * width, LANES), width)
        after = jnp.minimum(i + 1, chunks - 1)
        for k in range(len(steps)):
            if k + 1 < len(steps):
                ref, start = steps[k + 1]
                later = scores_into(scratch[(k + 1) % 2], ref, start, frames_of(i))
            else:
                ref, start = steps[0]
                later = scores_into(scratch[0], ref, start, frames_of(after))
            p = jnp.exp2((scratch[k % 2][...] - top) * LOG2E)
            probs[pl.ds(k * VB, VB), lanes] = p
            high[pl.ds(k, 1), lanes] = top
            total[pl.ds(k, 1), lanes] = jnp.sum(p, axis=0, keepdims=True)
            top = later
        return top

    first = scores_into(scratch[0], steps[0][0], steps[0][1], frames_of(0))
    lax.fori_loop(0, chunks, chunk, first)


def merged(high, total):
    top = jnp.max(high, axis=0, keepdims=True)
    return top + jnp.log(
        jnp.sum(total * jnp.exp(high - top), axis=0, keepdims=True)
    )


def own_kernel(line, c0, c1, c2, c3, probs, high, total, sa, sb):
    def frames_of(i):
        return line[pl.ds(0, FB), :]

    tile(frames_of, 1, FB, (c0, c1, c2, c3), probs, high, total, (sa, sb))


def near_kernel(before, after, c0, c1, c2, c3, probs, high, total, joined, sa, sb):
    count = before.shape[0]
    joined[pl.ds(0, count), :] = before[...]
    joined[pl.ds(count, count), :] = after[...]

    def frames_of(i):
        return joined[pl.ds(pl.multiple_of(i * FB, FB), FB), :]

    chunks = 2 * count // FB
    tile(frames_of, chunks, FB, (c0, c1, c2, c3), probs, high, total, (sa, sb))


def place(line, count):
    at = lax.rem(lax.axis_index("x") + line, lax.axis_size("x")) * count
    return pl.multiple_of(at, LANES)


def far_kernel(
    far, line, c0, c1, c2, c3, own_high, own_total, near_high, near_total,
    probs, high, lse_out, total, joined, sa, sb,
):
    count = far.shape[0]
    left = count - FB
    joined[pl.ds(0, count), :] = far[...]
    joined[pl.ds(count, left), :] = line[pl.ds(FB, left), :]

    def frames_of(i):
        return joined[pl.ds(pl.multiple_of(i * FB, FB), FB), :]

    chunks = (count + left) // FB
    tile(frames_of, chunks, FB, (c0, c1, c2, c3), probs, high, total, (sa, sb))

    def put(start, lse):
        lanes = pl.ds(start, lse.shape[1])
        for k in range(lse_out.shape[0]):
            lse_out[k, :, lanes] = lse

    put(place(0, count), merged(own_high[...], own_total[...]))
    near = merged(near_high[...], near_total[...])
    put(place(3, count), near[:, :count])
    put(place(1, count), near[:, count:])
    last = merged(high[...], total[...])
    put(place(2, count), last[:, :count])
    put(pl.multiple_of(place(0, count) + FB, LANES), last[:, count:])


def cost_of(count, protos, width):
    return pl.CostEstimate(
        flops=2 * count * protos * width,
        bytes_accessed=4 * count * protos,
        transcendentals=count * protos,
    )


def tile_call(kernel, tensors, codes, stats, count, last=None):
    width = codes[0].shape[1]
    protos = sum(c.shape[0] for c in codes)
    blocks = protos // VB
    f32, bf16 = jnp.float32, jnp.bfloat16
    stat = jax.ShapeDtypeStruct((blocks, count), f32)
    scratch = [pltpu.VMEM((VB, FB), f32)] * 2
    if len(tensors) > 1:
        scratch = [pltpu.VMEM((count, width), bf16)] + scratch
    if last is not None:
        scratch = [pltpu.VMEM((blocks, count), f32)] + scratch
    return pl.pallas_call(
        kernel,
        in_specs=in_vmem(len(tensors) + len(codes) + len(stats)),
        out_specs=in_vmem(3),
        out_shape=[
            jax.ShapeDtypeStruct((protos, count), f32),
            stat,
            stat if last is None else jax.ShapeDtypeStruct(last, f32),
        ],
        scratch_shapes=scratch,
        compiler_params=pltpu.CompilerParams(vmem_limit_bytes=8 * 1024 * 1024),
        cost_estimate=cost_of(count, protos, width),
    )(*tensors, *codes, *stats)


def usage_kernel(
    own_probs, own_high, near_probs, near_high, far_probs, far_high, parts,
    lse_out, usage_out,
):
    count = near_probs.shape[1] // 2
    left = count - FB
    groups = near_probs.shape[0] // LANES
    each = groups // 4
    peak = parts[0]
    for k in range(1, parts.shape[0]):
        peak = jnp.maximum(peak, parts[k])
    mass = jnp.exp(parts[0] - peak)
    for k in range(1, parts.shape[0]):
        mass = mass + jnp.exp(parts[k] - peak)
    lse_out[...] = peak + jnp.log(mass)

    yh, core = lax.axis_index("yh"), lax.axis_index("core")
    held = []

    def hold(probs, high, at, size, start):
        lse = lse_out[:, pl.ds(start, size)]
        held.append((probs, at, size, jnp.exp(high[:, at : at + size] - lse)))

    hold(own_probs, own_high, 0, FB, place(0, count))
    hold(near_probs, near_high, 0, count, place(3, count))
    hold(near_probs, near_high, count, count, place(1, count))
    hold(far_probs, far_high, 0, count, place(2, count))
    rest = pl.multiple_of(place(0, count) + FB, LANES)
    hold(far_probs, far_high, count, left, rest)

    for g in range(groups):
        block = g * LANES // VB
        acc = None
        for ref, at, size, weight in held:
            for j in range(0, size, LANES):
                term = (
                    ref[pl.ds(g * LANES, LANES), pl.ds(at + j, LANES)]
                    * weight[block : block + 1, j : j + LANES]
                )
                acc = term if acc is None else acc + term
        line = jnp.sum(acc.T, axis=0, keepdims=True)
        flip = g // each
        far, beside = flip // 2, flip % 2
        owner = jnp.where(yh == 1, 2 - 2 * far, 2 * far) + jnp.where(
            core == 1, 1 - beside, beside
        )
        for k in range(usage_out.shape[0]):
            usage_out[k, pl.ds(owner * each + g % each, 1), :] = line


def usage_of(held, parts, copies):
    protos = held[0].shape[0]
    total = parts.shape[2]
    f32 = jnp.float32
    return pl.pallas_call(
        usage_kernel,
        in_specs=in_vmem(len(held) + 1),
        out_specs=in_vmem(2),
        out_shape=[
            jax.ShapeDtypeStruct((1, total), f32),
            jax.ShapeDtypeStruct((copies, protos // LANES, LANES), f32),
        ],
        compiler_params=pltpu.CompilerParams(vmem_limit_bytes=8 * 1024 * 1024),
        cost_estimate=pl.CostEstimate(
            flops=2 * protos * total,
            bytes_accessed=4 * protos * total,
            transcendentals=total * protos // VB,
        ),
        name="usage_of",
    )(*held, parts)


def entropy_kernel(embeddings, counts, column_out, term_out):
    column = counts[0]
    for k in range(1, counts.shape[0]):
        column = column + counts[k]
    column_out[...] = column
    mean_use = column / embeddings
    term = -jnp.sum(mean_use * jnp.log(mean_use + 1e-07), keepdims=True)
    term_out[...] = jnp.broadcast_to(term[None], term_out.shape)


def entropy_of(counts, embeddings, copies):
    f32 = jnp.float32
    return pl.pallas_call(
        functools.partial(entropy_kernel, embeddings),
        in_specs=in_vmem(1),
        out_specs=in_vmem(2),
        out_shape=[
            jax.ShapeDtypeStruct(counts.shape[1:], f32),
            jax.ShapeDtypeStruct((copies, 1, LANES), f32),
        ],
        compiler_params=pltpu.CompilerParams(vmem_limit_bytes=4 * 1024 * 1024),
        name="entropy_of",
    )(counts)


def per_device(frames, codebook):
    own = frames[0]
    shard_rows, width = own.shape
    owned = codebook.shape[0]
    yh, core = lax.axis_index("yh"), lax.axis_index("core")
    plane, ring = lax.axis_size(PLANE), lax.axis_size(COLUMN)
    swap = [(0, 1), (1, 0)]

    opposite = lax.ppermute(codebook, RING_Y, [(0, 3), (3, 0), (1, 2), (2, 1)])
    beside = lax.ppermute(codebook, "core", swap)
    line = spread(own, "z").reshape(-1, width)
    far = shifted(line, 2)
    before = shifted(line, 1)
    after = shifted(line, -1)
    opposite, line = lax.optimization_barrier((opposite, line))
    across = lax.ppermute(opposite, "core", swap)

    count = line.shape[0]
    codes = (codebook, beside, opposite, across)
    own_probs, own_high, own_total = tile_call(
        own_kernel, (line,), codes, (), FB
    )
    near_probs, near_high, near_total = tile_call(
        near_kernel, (before, after), codes, (), 2 * count
    )
    stats = (own_high, own_total, near_high, near_total)
    far_probs, far_high, part = tile_call(
        far_kernel, (far, line), codes, stats, 2 * count - FB,
        (plane, 1, 4 * count),
    )
    parts = exchange(part, PLANE)
    held = (own_probs, own_high, near_probs, near_high, far_probs, far_high)
    lse, usage = usage_of(held, parts, ring)
    embeddings = shard_rows * lax.axis_size(BLK) * lax.axis_size("rep")
    column, term = entropy_of(exchange(usage, COLUMN), embeddings, plane)

    at = lax.axis_index(PLANE) * shard_rows
    lse_own = lax.dynamic_slice(lse, (0, at), (1, shard_rows))
    usage_own = lax.dynamic_slice_in_dim(
        column, (2 * yh + core) * (owned // LANES), owned // LANES, 0
    ).reshape(owned)
    entropy = jnp.sum(exchange(term, PLANE)[:, 0, 0])
    return (lse_own, usage_own, entropy)


def solution(mesh):
    split = Mesh(
        mesh.devices.reshape(4, 8, 2, 2, mesh.shape["rep"]),
        ("x", "z", "yh", "core", "rep"),
    )
    return jax.shard_map(
        per_device,
        mesh=split,
        in_specs=(P("rep", BLK, None), P(BLK, None)),
        out_specs=(P("rep", BLK), P(BLK), P()),
        check_vma=False,
    )
```

```python
import functools

import jax
import jax.numpy as jnp
from jax import lax
from jax.experimental import pallas as pl
from jax.experimental.pallas import tpu as pltpu
from jax.sharding import Mesh
from jax.sharding import PartitionSpec as P


BLK = ("x", "z", "yh", "core")
RING_Y = ("yh", "rep")
COLUMN = ("yh", "core", "rep")
PLANE = ("x", "z")
LOG2E = 1.4426950408889634
HELD = 256
LANES = 128


def exchange(array, axis):
    return lax.all_to_all(array, axis, split_axis=0, concat_axis=0, tiled=True)


def spread(array, axis):
    n = lax.axis_size(axis)
    return exchange(jnp.broadcast_to(array, (n, *array.shape)), axis)


def shifted(array, step):
    n = lax.axis_size("x")
    return lax.ppermute(array, "x", [(i, (i + step) % n) for i in range(n)])


def in_vmem(count):
    return [pl.BlockSpec(memory_space=pltpu.VMEM)] * count


def scores_into(scratch, codes, start, turned):
    s = jnp.dot(
        codes[pl.ds(start, scratch.shape[0]), :],
        turned[...],
        preferred_element_type=jnp.float32,
    )
    scratch[...] = s
    return jnp.max(s, axis=0, keepdims=True)


def tile(codes, turned, probs, high, total, scratch, home, arrival):
    fetch = pltpu.make_async_copy(codes[0], home, arrival)
    fetch.start()
    size = scratch[0].shape[0]
    steps = [
        (slot, start)
        for slot in (1, 2, 3, 0)
        for start in range(0, codes[slot].shape[0], size)
    ]

    def scores_at(k):
        slot, start = steps[k]
        if slot == 0 and start == 0:
            fetch.wait()
        ref = home if slot == 0 else codes[slot]
        return scores_into(scratch[k % 2], ref, start, turned)

    top = scores_at(0)
    for k in range(len(steps)):
        later = scores_at(k + 1) if k + 1 < len(steps) else None
        slot, start = steps[k]
        at = slot * home.shape[0] + start
        p = jnp.exp2((scratch[k % 2][...] - top) * LOG2E)
        probs[pl.ds(at, size), :] = p
        high[pl.ds(at // size, 1), :] = top
        total[pl.ds(at // size, 1), :] = jnp.sum(p, axis=0, keepdims=True)
        top = later


def merged(high, total):
    top = jnp.max(high, axis=0, keepdims=True)
    return top + jnp.log(
        jnp.sum(total * jnp.exp(high - top), axis=0, keepdims=True)
    )


def own_kernel(
    line, c0, c1, c2, c3, probs, high, total, turned, sa, sb, home, arrival
):
    turned[...] = line[pl.ds(0, HELD), :].T
    codes = (c0, c1, c2, c3)
    tile(codes, turned, probs, high, total, (sa, sb), home, arrival)


def join(pieces, joined, turned):
    at = 0
    for ref, start in pieces:
        size = ref.shape[0] - start
        joined[pl.ds(at, size), :] = ref[pl.ds(start, size), :]
        at += size
    turned[...] = joined[...].T


def near_kernel(
    b0, b1, a0, a1, c0, c1, c2, c3, probs, high, total,
    turned, sa, sb, home, arrival, joined,
):
    join([(b0, 0), (b1, 0), (a0, 0), (a1, 0)], joined, turned)
    codes = (c0, c1, c2, c3)
    tile(codes, turned, probs, high, total, (sa, sb), home, arrival)


def place(line, count):
    at = lax.rem(lax.axis_index("x") + line, lax.axis_size("x")) * count
    return pl.multiple_of(at, LANES)


def far_kernel(
    f0, f1, line, c0, c1, c2, c3, own_high, own_total, near_high, near_total,
    probs, high, lse_out, total, turned, sa, sb, home, arrival, joined,
):
    count = line.shape[0]
    join([(f0, 0), (f1, 0), (line, HELD)], joined, turned)
    codes = (c0, c1, c2, c3)
    tile(codes, turned, probs, high, total, (sa, sb), home, arrival)

    def put(start, lse):
        lanes = pl.ds(start, lse.shape[1])
        for k in range(lse_out.shape[0]):
            lse_out[k, :, lanes] = lse

    put(place(0, count), merged(own_high[...], own_total[...]))
    near = merged(near_high[...], near_total[...])
    put(place(3, count), near[:, :count])
    put(place(1, count), near[:, count:])
    last = merged(high[...], total[...])
    put(place(2, count), last[:, :count])
    put(pl.multiple_of(place(0, count) + HELD, LANES), last[:, count:])


def cost_of(count, protos, width):
    return pl.CostEstimate(
        flops=2 * count * protos * width,
        bytes_accessed=4 * count * protos,
        transcendentals=count * protos,
    )


def tile_call(kernel, tensors, codes, stats, count, size, last=None):
    width = codes[0].shape[1]
    protos = sum(c.shape[0] for c in codes)
    blocks = protos // size
    f32, bf16 = jnp.float32, jnp.bfloat16
    stat = jax.ShapeDtypeStruct((blocks, count), f32)
    scratch = [
        pltpu.VMEM((width, count), bf16),
        pltpu.VMEM((size, count), f32),
        pltpu.VMEM((size, count), f32),
        pltpu.VMEM(codes[0].shape, bf16),
        pltpu.SemaphoreType.DMA,
    ]
    if len(tensors) > 1:
        scratch = scratch + [pltpu.VMEM((count, width), bf16)]
    if last is not None:
        scratch = [pltpu.VMEM((blocks, count), f32)] + scratch
    home = pl.BlockSpec(memory_space=pltpu.HBM)
    others = in_vmem(len(codes) - 1 + len(stats))
    return pl.pallas_call(
        kernel,
        in_specs=in_vmem(len(tensors)) + [home] + others,
        out_specs=in_vmem(3),
        out_shape=[
            jax.ShapeDtypeStruct((protos, count), f32),
            stat,
            stat if last is None else jax.ShapeDtypeStruct(last, f32),
        ],
        scratch_shapes=scratch,
        compiler_params=pltpu.CompilerParams(vmem_limit_bytes=8 * 1024 * 1024),
        cost_estimate=cost_of(count, protos, width),
    )(*tensors, *codes, *stats)


def usage_kernel(
    own_probs, own_high, near_probs, near_high, far_probs, far_high, parts,
    lse_out, usage_out,
):
    count = near_probs.shape[1] // 2
    left = count - HELD
    groups = near_probs.shape[0] // LANES
    each = groups // 4
    peak = parts[0]
    for k in range(1, parts.shape[0]):
        peak = jnp.maximum(peak, parts[k])
    mass = jnp.exp(parts[0] - peak)
    for k in range(1, parts.shape[0]):
        mass = mass + jnp.exp(parts[k] - peak)
    lse_out[...] = peak + jnp.log(mass)

    yh, core = lax.axis_index("yh"), lax.axis_index("core")
    held = []

    def hold(probs, high, at, size, start):
        lse = lse_out[:, pl.ds(start, size)]
        weight = jnp.exp(high[:, at : at + size] - lse)
        held.append((probs, at, size, weight, probs.shape[0] // high.shape[0]))

    hold(own_probs, own_high, 0, HELD, place(0, count))
    hold(near_probs, near_high, 0, count, place(3, count))
    hold(near_probs, near_high, count, count, place(1, count))
    hold(far_probs, far_high, 0, count, place(2, count))
    rest = pl.multiple_of(place(0, count) + HELD, LANES)
    hold(far_probs, far_high, count, left, rest)

    for g in range(groups):
        acc = None
        for ref, at, size, weight, each_block in held:
            block = g * LANES // each_block
            for j in range(0, size, LANES):
                term = (
                    ref[pl.ds(g * LANES, LANES), pl.ds(at + j, LANES)]
                    * weight[block : block + 1, j : j + LANES]
                )
                acc = term if acc is None else acc + term
        line = jnp.sum(acc.T, axis=0, keepdims=True)
        flip = g // each
        far, beside = flip // 2, flip % 2
        owner = jnp.where(yh == 1, 2 - 2 * far, 2 * far) + jnp.where(
            core == 1, 1 - beside, beside
        )
        for k in range(usage_out.shape[0]):
            usage_out[k, pl.ds(owner * each + g % each, 1), :] = line


def usage_of(held, parts, copies):
    protos = held[0].shape[0]
    total = parts.shape[2]
    f32 = jnp.float32
    return pl.pallas_call(
        usage_kernel,
        in_specs=in_vmem(len(held) + 1),
        out_specs=in_vmem(2),
        out_shape=[
            jax.ShapeDtypeStruct((1, total), f32),
            jax.ShapeDtypeStruct((copies, protos // LANES, LANES), f32),
        ],
        compiler_params=pltpu.CompilerParams(vmem_limit_bytes=8 * 1024 * 1024),
        cost_estimate=pl.CostEstimate(
            flops=2 * protos * total,
            bytes_accessed=4 * protos * total,
            transcendentals=total * protos // LANES,
        ),
        name="usage_of",
    )(*held, parts)


def entropy_kernel(embeddings, counts, column_out, term_out):
    column = counts[0]
    for k in range(1, counts.shape[0]):
        column = column + counts[k]
    column_out[...] = column
    mean_use = column / embeddings
    term = -jnp.sum(mean_use * jnp.log(mean_use + 1e-07), keepdims=True)
    term_out[...] = jnp.broadcast_to(term[None], term_out.shape)


def entropy_of(counts, embeddings, copies):
    f32 = jnp.float32
    return pl.pallas_call(
        functools.partial(entropy_kernel, embeddings),
        in_specs=in_vmem(1),
        out_specs=in_vmem(2),
        out_shape=[
            jax.ShapeDtypeStruct(counts.shape[1:], f32),
            jax.ShapeDtypeStruct((copies, 1, LANES), f32),
        ],
        compiler_params=pltpu.CompilerParams(vmem_limit_bytes=4 * 1024 * 1024),
        name="entropy_of",
    )(counts)


def per_device(frames, codebook):
    own = frames[0]
    shard_rows, width = own.shape
    owned = codebook.shape[0]
    yh, core = lax.axis_index("yh"), lax.axis_index("core")
    plane, peers = lax.axis_size(PLANE), lax.axis_size(COLUMN)
    swap = [(0, 1), (1, 0)]

    ring = [(0, 3), (3, 0), (1, 2), (2, 1)]
    opposite = lax.ppermute(codebook, RING_Y, ring)
    beside = lax.ppermute(codebook, "core", swap)
    line = spread(own, "z").reshape(-1, width)
    count = line.shape[0]
    half = count // 2
    b0 = shifted(line[:half], 1)
    a1 = shifted(line[half:], -1)
    b1 = shifted(line[half:], 1)
    a0 = shifted(line[:half], -1)
    opposite, line = lax.optimization_barrier((opposite, line))
    across = lax.ppermute(opposite, "core", swap)
    f0 = shifted(b0, 1)
    f1 = shifted(a1, -1)
    home = pltpu.with_memory_space_constraint(codebook, pltpu.HBM)
    codes = (home, beside, opposite, across)
    own_probs, own_high, own_total = tile_call(
        own_kernel, (line,), codes, (), HELD, 256
    )
    near_probs, near_high, near_total = tile_call(
        near_kernel, (b0, b1, a0, a1), codes, (), 2 * count, 128
    )
    stats = (own_high, own_total, near_high, near_total)
    far_probs, far_high, part = tile_call(
        far_kernel, (f0, f1, line), codes, stats, 2 * count - HELD, 128,
        (plane, 1, 4 * count),
    )
    parts = exchange(part, PLANE)
    held = (own_probs, own_high, near_probs, near_high, far_probs, far_high)
    lse, usage = usage_of(held, parts, peers)
    embeddings = shard_rows * lax.axis_size(BLK) * lax.axis_size("rep")
    column, term = entropy_of(exchange(usage, COLUMN), embeddings, plane)

    at = lax.axis_index(PLANE) * shard_rows
    lse_own = lax.dynamic_slice(lse, (0, at), (1, shard_rows))
    usage_own = lax.dynamic_slice_in_dim(
        column, (2 * yh + core) * (owned // LANES), owned // LANES, 0
    ).reshape(owned)
    entropy = jnp.sum(exchange(term, PLANE)[:, 0, 0])
    return (lse_own, usage_own, entropy)


def solution(mesh):
    split = Mesh(
        mesh.devices.reshape(4, 8, 2, 2, mesh.shape["rep"]),
        ("x", "z", "yh", "core", "rep"),
    )
    return jax.shard_map(
        per_device,
        mesh=split,
        in_specs=(P("rep", BLK, None), P(BLK, None)),
        out_specs=(P("rep", BLK), P(BLK), P()),
        check_vma=False,
    )
```

```python
import functools

import jax
import jax.numpy as jnp
from jax import lax
from jax.experimental import pallas as pl
from jax.experimental.pallas import tpu as pltpu
from jax.sharding import Mesh
from jax.sharding import PartitionSpec as P


BLK = ("x", "z", "yh", "core")
RING_Y = ("yh", "rep")
COLUMN = ("yh", "core", "rep")
PLANE = ("x", "z")
LOG2E = 1.4426950408889634
HELD = 256
LANES = 128


def exchange(array, axis):
    return lax.all_to_all(array, axis, split_axis=0, concat_axis=0, tiled=True)


def spread(array, axis):
    n = lax.axis_size(axis)
    return exchange(jnp.broadcast_to(array, (n, *array.shape)), axis)


def shifted(array, step):
    n = lax.axis_size("x")
    return lax.ppermute(array, "x", [(i, (i + step) % n) for i in range(n)])


def in_vmem(count):
    return [pl.BlockSpec(memory_space=pltpu.VMEM)] * count


def scores_into(scratch, codes, start, turned):
    s = jnp.dot(
        codes[pl.ds(start, scratch.shape[0]), :],
        turned[...],
        preferred_element_type=jnp.float32,
    )
    scratch[:, pl.ds(0, turned.shape[1])] = s
    return jnp.max(s, axis=0, keepdims=True)


def tile(codes, turned, probs, high, total, scratch, home, arrival):
    fetch = pltpu.make_async_copy(codes[0], home, arrival)
    fetch.start()
    size = scratch[0].shape[0]
    steps = [
        (slot, start)
        for slot in (1, 2, 3, 0)
        for start in range(0, codes[slot].shape[0], size)
    ]

    def scores_at(k):
        slot, start = steps[k]
        if slot == 0 and start == 0:
            fetch.wait()
        ref = home if slot == 0 else codes[slot]
        return scores_into(scratch[k % 2], ref, start, turned)

    top = scores_at(0)
    for k in range(len(steps)):
        later = scores_at(k + 1) if k + 1 < len(steps) else None
        slot, start = steps[k]
        at = slot * home.shape[0] + start
        p = jnp.exp2((scratch[k % 2][:, pl.ds(0, probs.shape[1])] - top) * LOG2E)
        probs[pl.ds(at, size), :] = p
        high[pl.ds(at // size, 1), :] = top
        total[pl.ds(at // size, 1), :] = jnp.sum(p, axis=0, keepdims=True)
        top = later


def merged(high, total):
    top = jnp.max(high, axis=0, keepdims=True)
    return top + jnp.log(
        jnp.sum(total * jnp.exp(high - top), axis=0, keepdims=True)
    )


def turned_kernel(line, out):
    out[...] = line[pl.ds(0, out.shape[1]), :].T


def turned_of(line, count):
    return pl.pallas_call(
        turned_kernel,
        in_specs=in_vmem(1),
        out_specs=in_vmem(1)[0],
        out_shape=jax.ShapeDtypeStruct((line.shape[1], count), line.dtype),
        compiler_params=pltpu.CompilerParams(vmem_limit_bytes=4 * 1024 * 1024),
        name="turned_of",
    )(line)


def own_kernel(
    line, c0, c1, c2, c3, probs, high, total, turned, sa, sb, home, arrival
):
    turned[...] = line[...]
    codes = (c0, c1, c2, c3)
    tile(codes, turned, probs, high, total, (sa, sb), home, arrival)


def join(pieces, joined):
    at = 0
    for ref in pieces:
        joined[pl.ds(at, ref.shape[0]), :] = ref[...]
        at += ref.shape[0]


def near_kernel(
    b0, b1, a0, a1, c0, c1, c2, c3, probs, high, total,
    turned, sa, sb, home, arrival, joined,
):
    join((b0, b1, a0, a1), joined)
    turned[...] = joined[...].T
    codes = (c0, c1, c2, c3)
    tile(codes, turned, probs, high, total, (sa, sb), home, arrival)


def place(line, rows):
    return lax.rem(lax.axis_index("x") + line, lax.axis_size("x")) * rows


def far_kernel(
    f0, f1, line, c0, c1, c2, c3, own_high, own_total, near_high, near_total,
    probs, high, lse_out, dense, total, turned, sa, sb, home, arrival, joined,
):
    count = line.shape[0]
    join((f0, f1), joined)
    turned[:, pl.ds(0, count)] = joined[...].T
    turned[:, pl.ds(count, count - HELD)] = line[pl.ds(HELD, count - HELD), :].T
    codes = (c0, c1, c2, c3)
    tile(codes, turned, probs, high, total, (sa, sb), home, arrival)

    rows = count // LANES

    def put(row, lse):
        for j in range(lse.shape[1] // LANES):
            dense[pl.ds(row + j, 1), :] = lse[:, j * LANES : (j + 1) * LANES]

    put(place(0, rows), merged(own_high[...], own_total[...]))
    near = merged(near_high[...], near_total[...])
    put(place(3, rows), near[:, :count])
    put(place(1, rows), near[:, count:])
    last = merged(high[...], total[...])
    put(place(2, rows), last[:, :count])
    put(place(0, rows) + HELD // LANES, last[:, count:])
    lse = dense[...]
    twice = jnp.concatenate([lse, lse])
    step = twice.shape[0]
    for k in range(lse_out.shape[0] // step):
        lse_out[pl.ds(k * step, step), :] = twice


def cost_of(count, protos, width):
    return pl.CostEstimate(
        flops=2 * count * protos * width,
        bytes_accessed=4 * count * protos,
        transcendentals=count * protos,
    )


def tile_call(kernel, tensors, codes, stats, count, size, last=None):
    width = codes[0].shape[1]
    protos = sum(c.shape[0] for c in codes)
    blocks = protos // size
    f32, bf16 = jnp.float32, jnp.bfloat16
    stat = jax.ShapeDtypeStruct((blocks, count), f32)
    scratch = [
        pltpu.VMEM((size, count + LANES), f32),
        pltpu.VMEM((size, count + LANES), f32),
        pltpu.VMEM(codes[0].shape, bf16),
        pltpu.SemaphoreType.DMA,
    ]
    turned = pltpu.VMEM((width, count), bf16)
    scratch = [turned] + scratch
    if len(tensors) > 1:
        pieces = tensors if last is None else tensors[:2]
        held = sum(t.shape[0] for t in pieces)
        scratch = scratch + [pltpu.VMEM((held, width), bf16)]
    if last is not None:
        dense = pltpu.VMEM((last[0] // lax.axis_size(PLANE), LANES), f32)
        scratch = [dense, pltpu.VMEM((blocks, count), f32)] + scratch
    home = pl.BlockSpec(memory_space=pltpu.HBM)
    others = in_vmem(len(codes) - 1 + len(stats))
    return pl.pallas_call(
        kernel,
        in_specs=in_vmem(len(tensors)) + [home] + others,
        out_specs=in_vmem(3),
        out_shape=[
            jax.ShapeDtypeStruct((protos, count), f32),
            stat,
            stat if last is None else jax.ShapeDtypeStruct(last, f32),
        ],
        scratch_shapes=scratch,
        compiler_params=pltpu.CompilerParams(vmem_limit_bytes=8 * 1024 * 1024),
        cost_estimate=cost_of(count, protos, width),
    )(*tensors, *codes, *stats)


def usage_kernel(
    own_probs, own_high, near_probs, near_high, far_probs, far_high, parts,
    own_out, usage_out, lse_out, column,
):
    count = near_probs.shape[1] // 2
    left = count - HELD
    groups = near_probs.shape[0] // LANES
    each = groups // 4
    rows = count // LANES
    lines = lse_out.shape[0]
    pairs = range(0, parts.shape[0], 2 * lines)

    def both(combine, pair):
        return combine(pair[:lines], pair[lines:])

    peak = parts[pl.ds(0, 2 * lines), :]
    for k in pairs[1:]:
        peak = jnp.maximum(peak, parts[pl.ds(k, 2 * lines), :])
    peak = both(jnp.maximum, peak)
    twice = jnp.concatenate([peak, peak])
    mass = jnp.exp(parts[pl.ds(0, 2 * lines), :] - twice)
    for k in pairs[1:]:
        mass = mass + jnp.exp(parts[pl.ds(k, 2 * lines), :] - twice)
    lse_out[...] = peak + jnp.log(both(jnp.add, mass))

    shown = own_out.shape[1]
    at = lax.axis_index(PLANE) * shown
    row, shift = at // LANES, lax.rem(LANES - lax.rem(at, LANES), LANES)
    first = pltpu.roll(lse_out[pl.ds(row, 1), :], shift, 1)
    second = lse_out[pl.ds(jnp.minimum(row + 1, lines - 1), 1), :]
    second = pltpu.roll(second, shift, 1)
    lane = lax.broadcasted_iota(jnp.int32, (1, LANES), 1)
    straddle = jnp.logical_and(shift > 0, lane >= shift)
    own_out[...] = jnp.where(straddle, second, first)[:, :shown]

    yh, core = lax.axis_index("yh"), lax.axis_index("core")
    held = []

    def hold(probs, high, at, size, row):
        block = probs.shape[0] // high.shape[0]
        for j in range(0, size, LANES):
            lse = lse_out[pl.ds(row + j // LANES, 1), :]
            weight = jnp.exp(high[:, at + j : at + j + LANES] - lse)
            held.append((probs, at + j, weight, block))

    hold(own_probs, own_high, 0, HELD, place(0, rows))
    hold(near_probs, near_high, 0, count, place(3, rows))
    hold(near_probs, near_high, count, count, place(1, rows))
    hold(far_probs, far_high, 0, count, place(2, rows))
    hold(far_probs, far_high, count, left, place(0, rows) + HELD // LANES)

    for g in range(groups):
        acc = None
        for ref, at, weight, size in held:
            block = g * LANES // size
            row = jnp.broadcast_to(weight[block : block + 1, :], (8, LANES))
            probs = ref[pl.ds(g * LANES, LANES), pl.ds(at, LANES)]
            term = probs.reshape(-1, 8, LANES) * row
            acc = term if acc is None else acc + term
        acc = acc.reshape(LANES, LANES)
        line = jnp.sum(acc.T, axis=0, keepdims=True)
        flip = g // each
        far, beside = flip // 2, flip % 2
        owner = jnp.where(yh == 1, 2 - 2 * far, 2 * far) + jnp.where(
            core == 1, 1 - beside, beside
        )
        column[pl.ds(owner * each + g % each, 1), :] = line
    for k in range(usage_out.shape[0]):
        usage_out[k] = column[...]


def usage_of(held, parts, copies, shown):
    protos = held[0].shape[0]
    total = parts.shape[0] * LANES // lax.axis_size(PLANE)
    f32 = jnp.float32
    return pl.pallas_call(
        usage_kernel,
        in_specs=in_vmem(len(held) + 1),
        out_specs=in_vmem(2),
        out_shape=[
            jax.ShapeDtypeStruct((1, shown), f32),
            jax.ShapeDtypeStruct((copies, protos // LANES, LANES), f32),
        ],
        scratch_shapes=[
            pltpu.VMEM((total // LANES, LANES), f32),
            pltpu.VMEM((protos // LANES, LANES), f32),
        ],
        compiler_params=pltpu.CompilerParams(vmem_limit_bytes=8 * 1024 * 1024),
        cost_estimate=pl.CostEstimate(
            flops=2 * protos * total,
            bytes_accessed=4 * protos * total,
            transcendentals=total * protos // LANES,
        ),
        name="usage_of",
    )(*held, parts)


def entropy_kernel(embeddings, counts, own_out, term_out, column_out):
    column = counts[0]
    for k in range(1, counts.shape[0]):
        column = column + counts[k]
    column_out[...] = column
    slot = 2 * lax.axis_index("yh") + lax.axis_index("core")
    rows = own_out.shape[0]
    own_out[...] = column_out[pl.ds(pl.multiple_of(slot * rows, rows), rows), :]
    mean_use = column / embeddings
    term = -jnp.sum(mean_use * jnp.log(mean_use + 1e-07), keepdims=True)
    term_out[...] = jnp.broadcast_to(term[None], term_out.shape)


def entropy_of(counts, embeddings, copies):
    f32 = jnp.float32
    return pl.pallas_call(
        functools.partial(entropy_kernel, embeddings),
        in_specs=in_vmem(1),
        out_specs=in_vmem(2),
        out_shape=[
            jax.ShapeDtypeStruct((counts.shape[1] // 4, LANES), f32),
            jax.ShapeDtypeStruct((copies, 1, LANES), f32),
        ],
        scratch_shapes=[pltpu.VMEM(counts.shape[1:], f32)],
        compiler_params=pltpu.CompilerParams(vmem_limit_bytes=4 * 1024 * 1024),
        name="entropy_of",
    )(counts)


def per_device(frames, codebook):
    own = frames[0]
    shard_rows, width = own.shape
    owned = codebook.shape[0]
    plane, peers = lax.axis_size(PLANE), lax.axis_size(COLUMN)
    swap = [(0, 1), (1, 0)]

    ring = [(0, 3), (3, 0), (1, 2), (2, 1)]
    opposite = lax.ppermute(codebook, RING_Y, ring)
    beside = lax.ppermute(codebook, "core", swap)
    line = spread(own, "z").reshape(-1, width)
    count = line.shape[0]
    half = count // 2
    b0 = shifted(line[:half], 1)
    a1 = shifted(line[half:], -1)
    b1 = shifted(line[half:], 1)
    a0 = shifted(line[:half], -1)
    opposite, line = lax.optimization_barrier((opposite, line))
    across = lax.ppermute(opposite, "core", swap)
    f0 = shifted(b0, 1)
    f1 = shifted(a1, -1)
    home = pltpu.with_memory_space_constraint(codebook, pltpu.HBM)
    codes = (home, beside, opposite, across)
    turned = turned_of(line, HELD)
    own_probs, own_high, own_total = tile_call(
        own_kernel, (turned,), codes, (), HELD, 256
    )
    near_probs, near_high, near_total = tile_call(
        near_kernel, (b0, b1, a0, a1), codes, (), 2 * count, 128
    )
    stats = (own_high, own_total, near_high, near_total)
    far_probs, far_high, part = tile_call(
        far_kernel, (f0, f1, line), codes, stats, 2 * count - HELD, 128,
        (plane * 4 * count // LANES, LANES),
    )
    parts = exchange(part.reshape(plane, 1, 4 * count), PLANE).reshape(part.shape)
    held = (own_probs, own_high, near_probs, near_high, far_probs, far_high)
    lse_own, usage = usage_of(held, parts, peers, shard_rows)
    embeddings = shard_rows * lax.axis_size(BLK) * lax.axis_size("rep")
    usage_own, term = entropy_of(exchange(usage, COLUMN), embeddings, plane)
    entropy = jnp.sum(exchange(term, PLANE)[:, 0, 0])
    return (lse_own, usage_own.reshape(owned), entropy)


def solution(mesh):
    split = Mesh(
        mesh.devices.reshape(4, 8, 2, 2, mesh.shape["rep"]),
        ("x", "z", "yh", "core", "rep"),
    )
    return jax.shard_map(
        per_device,
        mesh=split,
        in_specs=(P("rep", BLK, None), P(BLK, None)),
        out_specs=(P("rep", BLK), P(BLK), P()),
        check_vma=False,
    )
```

```python
import functools

import jax
import jax.numpy as jnp
from jax import lax
from jax.experimental import pallas as pl
from jax.experimental.pallas import tpu as pltpu
from jax.sharding import Mesh
from jax.sharding import PartitionSpec as P


BLK = ("x", "z", "yh", "core")
RING_Y = ("yh", "rep")
COLUMN = ("yh", "core", "rep")
PLANE = ("x", "z")
LOG2E = 1.4426950408889634
HELD = 256
LANES = 128


def exchange(array, axis):
    return lax.all_to_all(array, axis, split_axis=0, concat_axis=0, tiled=True)


def spread(array, axis):
    n = lax.axis_size(axis)
    return exchange(jnp.broadcast_to(array, (n, *array.shape)), axis)


def shifted(array, step):
    n = lax.axis_size("x")
    return lax.ppermute(array, "x", [(i, (i + step) % n) for i in range(n)])


def in_vmem(count):
    return [pl.BlockSpec(memory_space=pltpu.VMEM)] * count


def scores_into(scratch, codes, start, turned):
    s = jnp.dot(
        codes[pl.ds(start, scratch.shape[0]), :],
        turned[...],
        preferred_element_type=jnp.float32,
    )
    scratch[:, pl.ds(0, turned.shape[1])] = s
    return jnp.max(s, axis=0, keepdims=True)


def tile(codes, turned, probs, high, total, scratch, home, arrival):
    fetch = pltpu.make_async_copy(codes[0], home, arrival)
    fetch.start()
    size = scratch[0].shape[0]
    steps = [
        (slot, start)
        for slot in (1, 2, 3, 0)
        for start in range(0, codes[slot].shape[0], size)
    ]

    def scores_at(k):
        slot, start = steps[k]
        if slot == 0 and start == 0:
            fetch.wait()
        ref = home if slot == 0 else codes[slot]
        return scores_into(scratch[k % 2], ref, start, turned)

    top = scores_at(0)
    for k in range(len(steps)):
        later = scores_at(k + 1) if k + 1 < len(steps) else None
        slot, start = steps[k]
        at = slot * home.shape[0] + start
        p = jnp.exp2((scratch[k % 2][:, pl.ds(0, probs.shape[1])] - top) * LOG2E)
        probs[pl.ds(at, size), :] = p
        high[pl.ds(at // size, 1), :] = top
        total[pl.ds(at // size, 1), :] = jnp.sum(p, axis=0, keepdims=True)
        top = later


def merged(high, total):
    top = jnp.max(high, axis=0, keepdims=True)
    return top + jnp.log(
        jnp.sum(total * jnp.exp(high - top), axis=0, keepdims=True)
    )


def turned_kernel(start, line, out):
    out[...] = line[pl.ds(start, out.shape[1]), :].T


def turned_of(line, start, count):
    return pl.pallas_call(
        functools.partial(turned_kernel, start),
        in_specs=in_vmem(1),
        out_specs=in_vmem(1)[0],
        out_shape=jax.ShapeDtypeStruct((line.shape[1], count), line.dtype),
        compiler_params=pltpu.CompilerParams(vmem_limit_bytes=4 * 1024 * 1024),
        name="turned_of",
    )(line)


def own_kernel(
    line, c0, c1, c2, c3, probs, high, total, turned, sa, sb, home, arrival
):
    turned[...] = line[...]
    codes = (c0, c1, c2, c3)
    tile(codes, turned, probs, high, total, (sa, sb), home, arrival)


def join(pieces, joined):
    at = 0
    for ref in pieces:
        joined[pl.ds(at, ref.shape[0]), :] = ref[...]
        at += ref.shape[0]


def near_kernel(
    b0, b1, a0, a1, c0, c1, c2, c3, probs, high, total,
    turned, sa, sb, home, arrival, joined,
):
    join((b0, b1, a0, a1), joined)
    turned[...] = joined[...].T
    codes = (c0, c1, c2, c3)
    tile(codes, turned, probs, high, total, (sa, sb), home, arrival)


def place(line, rows):
    return lax.rem(lax.axis_index("x") + line, lax.axis_size("x")) * rows


def far_kernel(
    f0, f1, left, c0, c1, c2, c3, own_high, own_total, near_high, near_total,
    probs, high, lse_out, dense, total, turned, sa, sb, home, arrival, joined,
):
    count = joined.shape[0]
    join((f0, f1), joined)
    turned[:, pl.ds(0, count)] = joined[...].T
    turned[:, pl.ds(count, count - HELD)] = left[...]
    codes = (c0, c1, c2, c3)
    tile(codes, turned, probs, high, total, (sa, sb), home, arrival)

    rows = count // LANES

    def put(row, lse):
        for j in range(lse.shape[1] // LANES):
            dense[pl.ds(row + j, 1), :] = lse[:, j * LANES : (j + 1) * LANES]

    put(place(0, rows), merged(own_high[...], own_total[...]))
    near = merged(near_high[...], near_total[...])
    put(place(3, rows), near[:, :count])
    put(place(1, rows), near[:, count:])
    last = merged(high[...], total[...])
    put(place(2, rows), last[:, :count])
    put(place(0, rows) + HELD // LANES, last[:, count:])
    lse = dense[...]
    twice = jnp.concatenate([lse, lse])
    step = twice.shape[0]
    for k in range(lse_out.shape[0] // step):
        lse_out[pl.ds(k * step, step), :] = twice


def cost_of(count, protos, width):
    return pl.CostEstimate(
        flops=2 * count * protos * width,
        bytes_accessed=4 * count * protos,
        transcendentals=count * protos,
    )


def tile_call(kernel, tensors, codes, stats, count, size, last=None):
    width = codes[0].shape[1]
    protos = sum(c.shape[0] for c in codes)
    blocks = protos // size
    f32, bf16 = jnp.float32, jnp.bfloat16
    stat = jax.ShapeDtypeStruct((blocks, count), f32)
    scratch = [
        pltpu.VMEM((size, count + LANES), f32),
        pltpu.VMEM((size, count + LANES), f32),
        pltpu.VMEM(codes[0].shape, bf16),
        pltpu.SemaphoreType.DMA,
    ]
    turned = pltpu.VMEM((width, count), bf16)
    scratch = [turned] + scratch
    if len(tensors) > 1:
        pieces = tensors if last is None else tensors[:2]
        held = sum(t.shape[0] for t in pieces)
        scratch = scratch + [pltpu.VMEM((held, width), bf16)]
    if last is not None:
        dense = pltpu.VMEM((last[0] // lax.axis_size(PLANE), LANES), f32)
        scratch = [dense, pltpu.VMEM((blocks, count), f32)] + scratch
    home = pl.BlockSpec(memory_space=pltpu.HBM)
    others = in_vmem(len(codes) - 1 + len(stats))
    return pl.pallas_call(
        kernel,
        in_specs=in_vmem(len(tensors)) + [home] + others,
        out_specs=in_vmem(3),
        out_shape=[
            jax.ShapeDtypeStruct((protos, count), f32),
            stat,
            stat if last is None else jax.ShapeDtypeStruct(last, f32),
        ],
        scratch_shapes=scratch,
        compiler_params=pltpu.CompilerParams(vmem_limit_bytes=8 * 1024 * 1024),
        cost_estimate=cost_of(count, protos, width),
    )(*tensors, *codes, *stats)


def usage_kernel(
    own_probs, own_high, near_probs, near_high, far_probs, far_high, parts,
    own_out, usage_out, lse_out, column,
):
    count = near_probs.shape[1] // 2
    left = count - HELD
    groups = near_probs.shape[0] // LANES
    each = groups // 4
    rows = count // LANES
    lines = lse_out.shape[0]
    pairs = range(0, parts.shape[0], 2 * lines)

    def both(combine, pair):
        return combine(pair[:lines], pair[lines:])

    peak = parts[pl.ds(0, 2 * lines), :]
    for k in pairs[1:]:
        peak = jnp.maximum(peak, parts[pl.ds(k, 2 * lines), :])
    peak = both(jnp.maximum, peak)
    twice = jnp.concatenate([peak, peak])
    mass = jnp.exp(parts[pl.ds(0, 2 * lines), :] - twice)
    for k in pairs[1:]:
        mass = mass + jnp.exp(parts[pl.ds(k, 2 * lines), :] - twice)
    lse_out[...] = peak + jnp.log(both(jnp.add, mass))

    shown = own_out.shape[1]
    at = lax.axis_index(PLANE) * shown
    row, shift = at // LANES, lax.rem(LANES - lax.rem(at, LANES), LANES)
    first = pltpu.roll(lse_out[pl.ds(row, 1), :], shift, 1)
    second = lse_out[pl.ds(jnp.minimum(row + 1, lines - 1), 1), :]
    second = pltpu.roll(second, shift, 1)
    lane = lax.broadcasted_iota(jnp.int32, (1, LANES), 1)
    straddle = jnp.logical_and(shift > 0, lane >= shift)
    own_out[...] = jnp.where(straddle, second, first)[:, :shown]

    yh, core = lax.axis_index("yh"), lax.axis_index("core")
    held = []

    def hold(probs, high, at, size, row):
        block = probs.shape[0] // high.shape[0]
        for j in range(0, size, LANES):
            lse = lse_out[pl.ds(row + j // LANES, 1), :]
            weight = jnp.exp(high[:, at + j : at + j + LANES] - lse)
            held.append((probs, at + j, weight, block))

    hold(own_probs, own_high, 0, HELD, place(0, rows))
    hold(near_probs, near_high, 0, count, place(3, rows))
    hold(near_probs, near_high, count, count, place(1, rows))
    hold(far_probs, far_high, 0, count, place(2, rows))
    hold(far_probs, far_high, count, left, place(0, rows) + HELD // LANES)

    for g in range(groups):
        acc = None
        for ref, at, weight, size in held:
            block = g * LANES // size
            row = jnp.broadcast_to(weight[block : block + 1, :], (8, LANES))
            probs = ref[pl.ds(g * LANES, LANES), pl.ds(at, LANES)]
            term = probs.reshape(-1, 8, LANES) * row
            acc = term if acc is None else acc + term
        acc = acc.reshape(LANES, LANES)
        line = jnp.sum(acc.T, axis=0, keepdims=True)
        flip = g // each
        far, beside = flip // 2, flip % 2
        owner = jnp.where(yh == 1, 2 - 2 * far, 2 * far) + jnp.where(
            core == 1, 1 - beside, beside
        )
        column[pl.ds(owner * each + g % each, 1), :] = line
    for k in range(usage_out.shape[0]):
        usage_out[k] = column[...]


def usage_of(held, parts, copies, shown):
    protos = held[0].shape[0]
    total = parts.shape[0] * LANES // lax.axis_size(PLANE)
    f32 = jnp.float32
    return pl.pallas_call(
        usage_kernel,
        in_specs=in_vmem(len(held) + 1),
        out_specs=in_vmem(2),
        out_shape=[
            jax.ShapeDtypeStruct((1, shown), f32),
            jax.ShapeDtypeStruct((copies, protos // LANES, LANES), f32),
        ],
        scratch_shapes=[
            pltpu.VMEM((total // LANES, LANES), f32),
            pltpu.VMEM((protos // LANES, LANES), f32),
        ],
        compiler_params=pltpu.CompilerParams(vmem_limit_bytes=8 * 1024 * 1024),
        cost_estimate=pl.CostEstimate(
            flops=2 * protos * total,
            bytes_accessed=4 * protos * total,
            transcendentals=total * protos // LANES,
        ),
        name="usage_of",
    )(*held, parts)


def entropy_kernel(embeddings, counts, own_out, term_out, column_out):
    column = counts[0]
    for k in range(1, counts.shape[0]):
        column = column + counts[k]
    column_out[...] = column
    slot = 2 * lax.axis_index("yh") + lax.axis_index("core")
    rows = own_out.shape[0]
    own_out[...] = column_out[pl.ds(pl.multiple_of(slot * rows, rows), rows), :]
    mean_use = column / embeddings
    term = -jnp.sum(mean_use * jnp.log(mean_use + 1e-07), keepdims=True)
    term_out[...] = jnp.broadcast_to(term[None], term_out.shape)


def entropy_of(counts, embeddings, copies):
    f32 = jnp.float32
    return pl.pallas_call(
        functools.partial(entropy_kernel, embeddings),
        in_specs=in_vmem(1),
        out_specs=in_vmem(2),
        out_shape=[
            jax.ShapeDtypeStruct((counts.shape[1] // 4, LANES), f32),
            jax.ShapeDtypeStruct((copies, 1, LANES), f32),
        ],
        scratch_shapes=[pltpu.VMEM(counts.shape[1:], f32)],
        compiler_params=pltpu.CompilerParams(vmem_limit_bytes=4 * 1024 * 1024),
        name="entropy_of",
    )(counts)


def per_device(frames, codebook):
    own = frames[0]
    shard_rows, width = own.shape
    owned = codebook.shape[0]
    plane, peers = lax.axis_size(PLANE), lax.axis_size(COLUMN)
    swap = [(0, 1), (1, 0)]

    ring = [(0, 3), (3, 0), (1, 2), (2, 1)]
    opposite = lax.ppermute(codebook, RING_Y, ring)
    beside = lax.ppermute(codebook, "core", swap)
    line = spread(own, "z").reshape(-1, width)
    count = line.shape[0]
    half = count // 2
    b0 = shifted(line[:half], 1)
    a1 = shifted(line[half:], -1)
    b1 = shifted(line[half:], 1)
    a0 = shifted(line[:half], -1)
    across = lax.ppermute(opposite, "core", swap)
    f0 = shifted(b0, 1)
    f1 = shifted(a1, -1)
    home = pltpu.with_memory_space_constraint(codebook, pltpu.HBM)
    codes = (home, beside, opposite, across)
    turned = turned_of(line, 0, HELD)
    left = turned_of(line, HELD, count - HELD)
    own_probs, own_high, own_total = tile_call(
        own_kernel, (turned,), codes, (), HELD, 256
    )
    near_probs, near_high, near_total = tile_call(
        near_kernel, (b0, b1, a0, a1), codes, (), 2 * count, 128
    )
    stats = (own_high, own_total, near_high, near_total)
    far_probs, far_high, part = tile_call(
        far_kernel, (f0, f1, left), codes, stats, 2 * count - HELD, 128,
        (plane * 4 * count // LANES, LANES),
    )
    parts = exchange(part.reshape(plane, 1, 4 * count), PLANE).reshape(part.shape)
    held = (own_probs, own_high, near_probs, near_high, far_probs, far_high)
    lse_own, usage = usage_of(held, parts, peers, shard_rows)
    embeddings = shard_rows * lax.axis_size(BLK) * lax.axis_size("rep")
    usage_own, term = entropy_of(exchange(usage, COLUMN), embeddings, plane)
    entropy = jnp.sum(exchange(term, PLANE)[:, 0, 0])
    return (lse_own, usage_own.reshape(owned), entropy)


def solution(mesh):
    split = Mesh(
        mesh.devices.reshape(4, 8, 2, 2, mesh.shape["rep"]),
        ("x", "z", "yh", "core", "rep"),
    )
    return jax.shard_map(
        per_device,
        mesh=split,
        in_specs=(P("rep", BLK, None), P(BLK, None)),
        out_specs=(P("rep", BLK), P(BLK), P()),
        check_vma=False,
    )
```

```python
import functools

import jax
import jax.numpy as jnp
from jax import lax
from jax.experimental import pallas as pl
from jax.experimental.pallas import tpu as pltpu
from jax.sharding import Mesh
from jax.sharding import PartitionSpec as P


BLK = ("x", "z", "yh", "core")
RING_Y = ("yh", "rep")
COLUMN = ("yh", "core", "rep")
PLANE = ("x", "z")
LOG2E = 1.4426950408889634
HELD = 256
LANES = 128


def exchange(array, axis):
    return lax.all_to_all(array, axis, split_axis=0, concat_axis=0, tiled=True)


def spread(array, axis):
    n = lax.axis_size(axis)
    return exchange(jnp.broadcast_to(array, (n, *array.shape)), axis)


def shifted(array, step):
    n = lax.axis_size("x")
    return lax.ppermute(array, "x", [(i, (i + step) % n) for i in range(n)])


def in_vmem(count):
    return [pl.BlockSpec(memory_space=pltpu.VMEM)] * count


def scores_into(scratch, codes, start, turned):
    s = jnp.dot(
        codes[pl.ds(start, scratch.shape[0]), :],
        turned[...],
        preferred_element_type=jnp.float32,
    )
    scratch[:, pl.ds(0, turned.shape[1])] = s
    return jnp.max(s, axis=0, keepdims=True)


def tile(codes, turned, probs, high, total, scratch, home, arrival):
    fetch = pltpu.make_async_copy(codes[0], home, arrival)
    fetch.start()
    size = scratch[0].shape[0]
    steps = [
        (slot, start)
        for slot in (1, 2, 3, 0)
        for start in range(0, codes[slot].shape[0], size)
    ]

    def scores_at(k):
        slot, start = steps[k]
        if slot == 0 and start == 0:
            fetch.wait()
        ref = home if slot == 0 else codes[slot]
        return scores_into(scratch[k % 2], ref, start, turned)

    top = scores_at(0)
    for k in range(len(steps)):
        later = scores_at(k + 1) if k + 1 < len(steps) else None
        slot, start = steps[k]
        at = slot * home.shape[0] + start
        p = jnp.exp2((scratch[k % 2][:, pl.ds(0, probs.shape[1])] - top) * LOG2E)
        probs[pl.ds(at, size), :] = p
        high[pl.ds(at // size, 1), :] = top
        total[pl.ds(at // size, 1), :] = jnp.sum(p, axis=0, keepdims=True)
        top = later


def merged(high, total):
    top = jnp.max(high, axis=0, keepdims=True)
    return top + jnp.log(
        jnp.sum(total * jnp.exp(high - top), axis=0, keepdims=True)
    )


def turned_kernel(line, out):
    out[...] = line[pl.ds(0, out.shape[1]), :].T


def turned_of(line, count):
    return pl.pallas_call(
        turned_kernel,
        in_specs=in_vmem(1),
        out_specs=in_vmem(1)[0],
        out_shape=jax.ShapeDtypeStruct((line.shape[1], count), line.dtype),
        compiler_params=pltpu.CompilerParams(vmem_limit_bytes=4 * 1024 * 1024),
        name="turned_of",
    )(line)


def own_kernel(
    line, c0, c1, c2, c3, probs, high, total, turned, sa, sb, home, arrival
):
    turned[...] = line[...]
    codes = (c0, c1, c2, c3)
    tile(codes, turned, probs, high, total, (sa, sb), home, arrival)


def join(pieces, joined):
    at = 0
    for ref in pieces:
        joined[pl.ds(at, ref.shape[0]), :] = ref[...]
        at += ref.shape[0]


def near_kernel(
    b0, b1, a0, a1, c0, c1, c2, c3, probs, high, total,
    turned, sa, sb, home, arrival, joined,
):
    join((b0, b1, a0, a1), joined)
    turned[...] = joined[...].T
    codes = (c0, c1, c2, c3)
    tile(codes, turned, probs, high, total, (sa, sb), home, arrival)


def place(line, rows):
    return lax.rem(lax.axis_index("x") + line, lax.axis_size("x")) * rows


def far_kernel(
    f0, f1, line, c0, c1, c2, c3, own_high, own_total, near_high, near_total,
    probs, high, lse_out, dense, total, turned, sa, sb, home, arrival, joined,
):
    count = line.shape[0]
    join((f0, f1), joined)
    turned[:, pl.ds(0, count)] = joined[...].T
    turned[:, pl.ds(count, count - HELD)] = line[pl.ds(HELD, count - HELD), :].T
    codes = (c0, c1, c2, c3)
    tile(codes, turned, probs, high, total, (sa, sb), home, arrival)

    rows = count // LANES

    def put(row, lse):
        for j in range(lse.shape[1] // LANES):
            dense[pl.ds(row + j, 1), :] = lse[:, j * LANES : (j + 1) * LANES]

    put(place(0, rows), merged(own_high[...], own_total[...]))
    near = merged(near_high[...], near_total[...])
    put(place(3, rows), near[:, :count])
    put(place(1, rows), near[:, count:])
    last = merged(high[...], total[...])
    put(place(2, rows), last[:, :count])
    put(place(0, rows) + HELD // LANES, last[:, count:])
    lse = dense[...]
    twice = jnp.concatenate([lse, lse])
    step = twice.shape[0]
    for k in range(lse_out.shape[0] // step):
        lse_out[pl.ds(k * step, step), :] = twice


def cost_of(count, protos, width):
    return pl.CostEstimate(
        flops=2 * count * protos * width,
        bytes_accessed=4 * count * protos,
        transcendentals=count * protos,
    )


def tile_call(kernel, tensors, codes, stats, count, size, last=None):
    width = codes[0].shape[1]
    protos = sum(c.shape[0] for c in codes)
    blocks = protos // size
    f32, bf16 = jnp.float32, jnp.bfloat16
    stat = jax.ShapeDtypeStruct((blocks, count), f32)
    scratch = [
        pltpu.VMEM((size, count + LANES), f32),
        pltpu.VMEM((size, count + LANES), f32),
        pltpu.VMEM(codes[0].shape, bf16),
        pltpu.SemaphoreType.DMA,
    ]
    turned = pltpu.VMEM((width, count), bf16)
    scratch = [turned] + scratch
    if len(tensors) > 1:
        pieces = tensors if last is None else tensors[:2]
        held = sum(t.shape[0] for t in pieces)
        scratch = scratch + [pltpu.VMEM((held, width), bf16)]
    if last is not None:
        dense = pltpu.VMEM((last[0] // lax.axis_size(PLANE), LANES), f32)
        scratch = [dense, pltpu.VMEM((blocks, count), f32)] + scratch
    home = pl.BlockSpec(memory_space=pltpu.HBM)
    others = in_vmem(len(codes) - 1 + len(stats))
    return pl.pallas_call(
        kernel,
        in_specs=in_vmem(len(tensors)) + [home] + others,
        out_specs=in_vmem(3),
        out_shape=[
            jax.ShapeDtypeStruct((protos, count), f32),
            stat,
            stat if last is None else jax.ShapeDtypeStruct(last, f32),
        ],
        scratch_shapes=scratch,
        compiler_params=pltpu.CompilerParams(vmem_limit_bytes=8 * 1024 * 1024),
        cost_estimate=cost_of(count, protos, width),
    )(*tensors, *codes, *stats)


def usage_kernel(
    own_probs, own_high, near_probs, near_high, far_probs, far_high, parts,
    own_out, usage_out, lse_out, column, shown_lse, leaving,
):
    count = near_probs.shape[1] // 2
    left = count - HELD
    groups = near_probs.shape[0] // LANES
    each = groups // 4
    rows = count // LANES
    lines = lse_out.shape[0]
    pairs = range(0, parts.shape[0], 2 * lines)

    def both(combine, pair):
        return combine(pair[:lines], pair[lines:])

    peak = parts[pl.ds(0, 2 * lines), :]
    for k in pairs[1:]:
        peak = jnp.maximum(peak, parts[pl.ds(k, 2 * lines), :])
    peak = both(jnp.maximum, peak)
    twice = jnp.concatenate([peak, peak])
    mass = jnp.exp(parts[pl.ds(0, 2 * lines), :] - twice)
    for k in pairs[1:]:
        mass = mass + jnp.exp(parts[pl.ds(k, 2 * lines), :] - twice)
    lse_out[...] = peak + jnp.log(both(jnp.add, mass))

    shown = shown_lse.shape[1]
    at = lax.axis_index(PLANE) * shown
    row, shift = at // LANES, lax.rem(LANES - lax.rem(at, LANES), LANES)
    first = pltpu.roll(lse_out[pl.ds(row, 1), :], shift, 1)
    second = lse_out[pl.ds(jnp.minimum(row + 1, lines - 1), 1), :]
    second = pltpu.roll(second, shift, 1)
    lane = lax.broadcasted_iota(jnp.int32, (1, LANES), 1)
    straddle = jnp.logical_and(shift > 0, lane >= shift)
    shown_lse[...] = jnp.where(straddle, second, first)[:, :shown]
    leave = pltpu.make_async_copy(shown_lse, own_out, leaving)
    leave.start()

    yh, core = lax.axis_index("yh"), lax.axis_index("core")
    held = []

    def hold(probs, high, at, size, row):
        block = probs.shape[0] // high.shape[0]
        for j in range(0, size, LANES):
            lse = lse_out[pl.ds(row + j // LANES, 1), :]
            weight = jnp.exp(high[:, at + j : at + j + LANES] - lse)
            held.append((probs, at + j, weight, block))

    hold(own_probs, own_high, 0, HELD, place(0, rows))
    hold(near_probs, near_high, 0, count, place(3, rows))
    hold(near_probs, near_high, count, count, place(1, rows))
    hold(far_probs, far_high, 0, count, place(2, rows))
    hold(far_probs, far_high, count, left, place(0, rows) + HELD // LANES)

    for g in range(groups):
        acc = None
        for ref, at, weight, size in held:
            block = g * LANES // size
            row = jnp.broadcast_to(weight[block : block + 1, :], (8, LANES))
            probs = ref[pl.ds(g * LANES, LANES), pl.ds(at, LANES)]
            term = probs.reshape(-1, 8, LANES) * row
            acc = term if acc is None else acc + term
        acc = acc.reshape(LANES, LANES)
        line = jnp.sum(acc.T, axis=0, keepdims=True)
        flip = g // each
        far, beside = flip // 2, flip % 2
        owner = jnp.where(yh == 1, 2 - 2 * far, 2 * far) + jnp.where(
            core == 1, 1 - beside, beside
        )
        column[pl.ds(owner * each + g % each, 1), :] = line
    for k in range(usage_out.shape[0]):
        usage_out[k] = column[...]
    leave.wait()


def usage_of(held, parts, copies, shown):
    protos = held[0].shape[0]
    total = parts.shape[0] * LANES // lax.axis_size(PLANE)
    f32 = jnp.float32
    return pl.pallas_call(
        usage_kernel,
        in_specs=in_vmem(len(held) + 1),
        out_specs=[pl.BlockSpec(memory_space=pltpu.HBM)] + in_vmem(1),
        out_shape=[
            jax.ShapeDtypeStruct((1, shown), f32),
            jax.ShapeDtypeStruct((copies, protos // LANES, LANES), f32),
        ],
        scratch_shapes=[
            pltpu.VMEM((total // LANES, LANES), f32),
            pltpu.VMEM((protos // LANES, LANES), f32),
            pltpu.VMEM((1, shown), f32),
            pltpu.SemaphoreType.DMA,
        ],
        compiler_params=pltpu.CompilerParams(vmem_limit_bytes=8 * 1024 * 1024),
        cost_estimate=pl.CostEstimate(
            flops=2 * protos * total,
            bytes_accessed=4 * protos * total,
            transcendentals=total * protos // LANES,
        ),
        name="usage_of",
    )(*held, parts)


def entropy_kernel(embeddings, counts, own_out, term_out, column_out):
    column = counts[0]
    for k in range(1, counts.shape[0]):
        column = column + counts[k]
    column_out[...] = column
    slot = 2 * lax.axis_index("yh") + lax.axis_index("core")
    rows = own_out.shape[0]
    own_out[...] = column_out[pl.ds(pl.multiple_of(slot * rows, rows), rows), :]
    mean_use = column / embeddings
    term = -jnp.sum(mean_use * jnp.log(mean_use + 1e-07), keepdims=True)
    term_out[...] = jnp.broadcast_to(term[None], term_out.shape)


def entropy_of(counts, embeddings, copies):
    f32 = jnp.float32
    return pl.pallas_call(
        functools.partial(entropy_kernel, embeddings),
        in_specs=in_vmem(1),
        out_specs=in_vmem(2),
        out_shape=[
            jax.ShapeDtypeStruct((counts.shape[1] // 4, LANES), f32),
            jax.ShapeDtypeStruct((copies, 1, LANES), f32),
        ],
        scratch_shapes=[pltpu.VMEM(counts.shape[1:], f32)],
        compiler_params=pltpu.CompilerParams(vmem_limit_bytes=4 * 1024 * 1024),
        name="entropy_of",
    )(counts)


def per_device(frames, codebook):
    own = frames[0]
    shard_rows, width = own.shape
    owned = codebook.shape[0]
    plane, peers = lax.axis_size(PLANE), lax.axis_size(COLUMN)
    swap = [(0, 1), (1, 0)]

    ring = [(0, 3), (3, 0), (1, 2), (2, 1)]
    opposite = lax.ppermute(codebook, RING_Y, ring)
    beside = lax.ppermute(codebook, "core", swap)
    line = spread(own, "z").reshape(-1, width)
    count = line.shape[0]
    half = count // 2
    b0 = shifted(line[:half], 1)
    a1 = shifted(line[half:], -1)
    b1 = shifted(line[half:], 1)
    a0 = shifted(line[:half], -1)
    opposite, line = lax.optimization_barrier((opposite, line))
    across = lax.ppermute(opposite, "core", swap)
    f0 = shifted(b0, 1)
    f1 = shifted(a1, -1)
    home = pltpu.with_memory_space_constraint(codebook, pltpu.HBM)
    codes = (home, beside, opposite, across)
    turned = turned_of(line, HELD)
    own_probs, own_high, own_total = tile_call(
        own_kernel, (turned,), codes, (), HELD, 256
    )
    near_probs, near_high, near_total = tile_call(
        near_kernel, (b0, b1, a0, a1), codes, (), 2 * count, 128
    )
    stats = (own_high, own_total, near_high, near_total)
    far_probs, far_high, part = tile_call(
        far_kernel, (f0, f1, line), codes, stats, 2 * count - HELD, 128,
        (plane * 4 * count // LANES, LANES),
    )
    parts = exchange(part.reshape(plane, 1, 4 * count), PLANE).reshape(part.shape)
    held = (own_probs, own_high, near_probs, near_high, far_probs, far_high)
    lse_own, usage = usage_of(held, parts, peers, shard_rows)
    embeddings = shard_rows * lax.axis_size(BLK) * lax.axis_size("rep")
    usage_own, term = entropy_of(exchange(usage, COLUMN), embeddings, plane)
    entropy = jnp.sum(exchange(term, PLANE)[:, 0, 0])
    return (lse_own, usage_own.reshape(owned), entropy)


def solution(mesh):
    split = Mesh(
        mesh.devices.reshape(4, 8, 2, 2, mesh.shape["rep"]),
        ("x", "z", "yh", "core", "rep"),
    )
    return jax.shard_map(
        per_device,
        mesh=split,
        in_specs=(P("rep", BLK, None), P(BLK, None)),
        out_specs=(P("rep", BLK), P(BLK), P()),
        check_vma=False,
    )
```
